256 devices in a mesh: dp: 64 (over x, z, y_hi), mp: 4 (over y_lo, core).
Axes of the slice: x: 4, y: 4 (y_hi: 2, y_lo: 2; y = y_hi * 2 + y_lo), z: 8, core: 2. Of those that a mesh axis runs over, the one named last changes fastest.
Arguments:
- media: bfloat16 [128, 8, 256, 1024], P('dp'), may hold values from -6 to 6
- latents: bfloat16 [64, 1024], replicated, may hold values from -6 to 6
- time_embed: bfloat16 [8, 1024], replicated, may hold values from -5 to 5
- media_gain: float32 [2, 1024], replicated, may hold values from 0.25 to 1.75
- latent_gain: float32 [2, 1024], replicated, may hold values from 0.25 to 1.75
- ffn_gain: float32 [2, 1024], replicated, may hold values from 0.25 to 1.75
- out_gain: float32 [1024], replicated, may hold values from 0.25 to 1.75
- w_query: bfloat16 [2, 1024, 512], P(None, 'dp', 'mp'), may hold values from -0.1875 to 0.1875
- w_key: bfloat16 [2, 1024, 512], P(None, 'dp', 'mp'), may hold values from -0.1875 to 0.1875
- w_value: bfloat16 [2, 1024, 512], P(None, 'dp', 'mp'), may hold values from -0.1875 to 0.1875
- w_out: bfloat16 [2, 512, 1024], P(None, 'mp', 'dp'), may hold values from -0.25 to 0.25
- w_up: bfloat16 [2, 1024, 4096], P(None, 'dp', 'mp'), may hold values from -0.1875 to 0.1875
- w_down: bfloat16 [2, 4096, 1024], P(None, 'mp', 'dp'), may hold values from -0.09375 to 0.09375
Outputs:
- resampled: bfloat16 [128, 64, 1024], P('dp')
The draws below stay inside these ranges and needn't reach their ends.
All inputs are finite; a program needn't handle non-finite values.
Results may differ from the reference program's by a relative error of at most 0.013.
Values may be sent and summed in bfloat16 or wider, within the bound.
No kernel may reach another device: no remote copies, remote signals or barrier semaphores. Data moves between devices by JAX's collectives and lax.ppermute only.
A program may use at most 128 MiB of HBM per device.

```python
import jax
import jax.numpy as jnp
from jax import lax

D = 1024
HEADS = 8
HEAD = 64
FF = 4096
NLAT = 64
FRAMES = 8
PATCHES = 256
LAYERS = 2
INNER = 512
SAMPLES = 128


def levels(stream_key, extent, cuts, low, largest):
    level, own = 1.0, jax.random.fold_in(stream_key, 6)
    for dim, shards_of in cuts:
        steps = jnp.exp(jax.random.uniform(jax.random.fold_in(own, dim), (shards_of,), jnp.float32, low / len(cuts), largest / len(cuts)))
        level = level * jnp.repeat(steps, extent[dim] // shards_of).reshape([-1 if axis == dim else 1 for axis in range(len(extent))])
    return level


def bell_draw(own_key, dims, scale, limit, cuts=(), dtype=jnp.bfloat16):
    entries = scale * jax.random.normal(own_key, dims, jnp.float32)
    if cuts:
        entries = entries * levels(own_key, dims, cuts, -0.22, 0.18)
    return jnp.clip(entries, -limit, limit).astype(dtype)


def setup_inputs(seed: int = 0) -> dict:
    key_of = jax.random.split(jax.random.key(seed), 14)
    return {
        "media": bell_draw(key_of[0], (SAMPLES, FRAMES, PATCHES, D), 1.0, 6.0, ((0, 64),)),
        "latents": bell_draw(key_of[1], (NLAT, D), 1.0, 6.0),
        "time_embed": bell_draw(key_of[2], (FRAMES, D), 0.7, 5.0),
        "media_gain": jnp.clip(1.0 + 0.15 * jax.random.normal(key_of[3], (LAYERS, D), jnp.float32), 0.25, 1.75),
        "latent_gain": jnp.clip(1.0 + 0.15 * jax.random.normal(key_of[4], (LAYERS, D), jnp.float32), 0.25, 1.75),
        "ffn_gain": jnp.clip(1.0 + 0.15 * jax.random.normal(key_of[5], (LAYERS, D), jnp.float32), 0.25, 1.75),
        "out_gain": jnp.clip(1.0 + 0.15 * jax.random.normal(key_of[6], (D,), jnp.float32), 0.25, 1.75),
        "w_query": bell_draw(key_of[7], (LAYERS, D, INNER), D ** -0.5, 0.1875, ((1, 64), (2, 4))),
        "w_key": bell_draw(key_of[8], (LAYERS, D, INNER), D ** -0.5, 0.1875, ((1, 64), (2, 4))),
        "w_value": bell_draw(key_of[9], (LAYERS, D, INNER), D ** -0.5, 0.1875, ((1, 64), (2, 4))),
        "w_out": bell_draw(key_of[10], (LAYERS, INNER, D), INNER ** -0.5, 0.25, ((1, 4), (2, 64))),
        "w_up": bell_draw(key_of[11], (LAYERS, D, FF), D ** -0.5, 0.1875, ((1, 64), (2, 4))),
        "w_down": bell_draw(key_of[12], (LAYERS, FF, D), FF ** -0.5, 0.09375, ((1, 4), (2, 64))),
    }


def layer_norm(values, gain):
    center = values - lax.optimization_barrier(jnp.mean(values, axis=-1, keepdims=True))
    spread = lax.optimization_barrier(jnp.mean(center * center, axis=-1, keepdims=True))
    return center * lax.rsqrt(spread + 1e-05) * gain

def reference(media, latents, time_embed, media_gain, latent_gain, ffn_gain, out_gain, w_query, w_key, w_value, w_out, w_up, w_down):
    scale = HEAD ** (-0.5)

    def one_sample(sample):
        flat = (sample.astype(jnp.float32) + time_embed.astype(jnp.float32)[:, None, :]).reshape(FRAMES * PATCHES, D)
        state = latents.astype(jnp.float32)
        for layer in range(LAYERS):
            media_normed = layer_norm(flat, media_gain[layer]).astype(jnp.bfloat16)
            latent_normed = layer_norm(state, latent_gain[layer]).astype(jnp.bfloat16)
            queries = (jnp.dot(latent_normed, w_query[layer], preferred_element_type=jnp.float32) * scale).astype(jnp.bfloat16)
            inputs = jnp.concatenate([media_normed, latent_normed], axis=0)
            keys = jnp.dot(inputs, w_key[layer], preferred_element_type=jnp.float32).astype(jnp.bfloat16)
            values = jnp.dot(inputs, w_value[layer], preferred_element_type=jnp.float32).astype(jnp.bfloat16)
            qheads = queries.astype(jnp.float32).reshape(NLAT, HEADS, HEAD)
            kheads = keys.astype(jnp.float32).reshape(-1, HEADS, HEAD)
            vheads = values.astype(jnp.float32).reshape(-1, HEADS, HEAD)
            scores = jnp.einsum('qhd,khd->hqk', qheads, kheads)
            probs = jax.nn.softmax(scores, axis=-1).astype(jnp.bfloat16)
            attended = jnp.einsum('hqk,khd->qhd', probs.astype(jnp.float32), vheads).astype(jnp.bfloat16).reshape(NLAT, HEADS * HEAD)
            state = state + jnp.dot(attended, w_out[layer], preferred_element_type=jnp.float32)
            ffn_normed = layer_norm(state, ffn_gain[layer]).astype(jnp.bfloat16)
            hidden = jax.nn.gelu(jnp.dot(ffn_normed, w_up[layer], preferred_element_type=jnp.float32), approximate=False).astype(jnp.bfloat16)
            state = state + jnp.dot(hidden, w_down[layer], preferred_element_type=jnp.float32)
        return layer_norm(state, out_gain).astype(jnp.bfloat16)
    return lax.map(one_sample, media)
```

```python
import jax
import jax.numpy as jnp
from jax import lax
from jax.experimental import pallas as pl
from jax.experimental.pallas import tpu as pltpu
from jax.sharding import Mesh, PartitionSpec as P

HEAD = 64
LAYERS = 2
CHUNK = 512
F32, BF16 = jnp.float32, jnp.bfloat16
DP = ("x", "z", "yh")
MP = ("yl", "c")


def params(**kw):
    return pltpu.CompilerParams(vmem_limit_bytes=60 * 1024 * 1024, **kw)


def norm(v, g):
    center = v - jnp.mean(v, axis=-1, keepdims=True)
    spread = jnp.mean(center * center, axis=-1, keepdims=True)
    return center * lax.rsqrt(spread + 1e-05) * g


def dot(a, b, dims=((1,), (0,))):
    return lax.dot_general(a, b, (dims, ((), ())), preferred_element_type=F32)


def for_everyone(x, axes, n):
    copies = jnp.broadcast_to(x, (n, *x.shape))
    return lax.all_to_all(copies, axes, split_axis=0, concat_axis=0, tiled=True)


def ring_pairs(n, step):
    return [(i, (i + step) % n) for i in range(n)]


def media_kernel(m_ref, t_ref, g_ref, o0_ref, o1_ref):
    flat = m_ref[0, 0].astype(F32) + t_ref[0].astype(F32)
    center = flat - jnp.mean(flat, axis=-1, keepdims=True)
    spread = jnp.mean(center * center, axis=-1, keepdims=True)
    unit = center * lax.rsqrt(spread + 1e-05)
    o0_ref[0] = (unit * g_ref[0:1, :]).astype(BF16)
    o1_ref[0] = (unit * g_ref[1:2, :]).astype(BF16)


def norm_media(media, time_embed, gains):
    s, f, p, d = media.shape
    out = jax.ShapeDtypeStruct((s, f * p, d), BF16)
    return pl.pallas_call(
        media_kernel,
        grid=(s, f),
        in_specs=[
            pl.BlockSpec((1, 1, p, d), lambda i, j: (i, j, 0, 0)),
            pl.BlockSpec((1, 1, d), lambda i, j: (j, 0, 0)),
            pl.BlockSpec((2, d), lambda i, j: (0, 0)),
        ],
        out_specs=[pl.BlockSpec((1, p, d), lambda i, j: (i, j, 0))] * 2,
        out_shape=[out, out],
        compiler_params=params(),
        cost_estimate=pl.CostEstimate(flops=4 * 10**9, bytes_accessed=24 * 2**20, transcendentals=0),
        name="norm_media",
    )(media, time_embed.reshape(f, 1, d), gains)


def attention_kernel(m_ref, s_ref, g_ref, w_ref, o_ref, kv_w, q_bd, score, vals):
    i, j = pl.program_id(0), pl.program_id(1)
    n_chunks = pl.num_programs(1)
    d = m_ref.shape[2]
    tokens = n_chunks * CHUNK
    lat = s_ref.shape[1]

    @pl.when((i == 0) & (j == 0))
    def _():
        kv_w[:, :128] = w_ref[:, 1].reshape(d, 128)
        kv_w[:, 128:] = w_ref[:, 2].reshape(d, 128)

    @pl.when(j == 0)
    def _():
        ln = norm(s_ref[0], g_ref[...]).astype(BF16)
        q = (dot(ln, w_ref[:, 0].reshape(d, 128)) * (HEAD**-0.5)).astype(BF16).astype(F32)
        qt = q.T
        both = jnp.concatenate([qt, qt], axis=1)
        row = lax.broadcasted_iota(jnp.int32, both.shape, 0) < HEAD
        col = lax.broadcasted_iota(jnp.int32, both.shape, 1) < lat
        q_bd[...] = jnp.where(row == col, both, 0.0).astype(BF16)
        kv = dot(ln, kv_w[...]).astype(BF16)
        score[pl.ds(tokens, lat), :] = dot(kv[:, :128], q_bd[...])
        vals[pl.ds(tokens, lat), :] = kv[:, 128:]

    kv = dot(m_ref[0], kv_w[...]).astype(BF16)
    at = pl.multiple_of(j * CHUNK, CHUNK)
    score[pl.ds(at, CHUNK), :] = dot(kv[:, :128], q_bd[...])
    vals[pl.ds(at, CHUNK), :] = kv[:, 128:]

    @pl.when(j == n_chunks - 1)
    def _():
        sc = score[...]
        e = jnp.exp(sc - jnp.max(sc, axis=0, keepdims=True))
        probs = (e / jnp.sum(e, axis=0, keepdims=True)).astype(BF16)
        att = dot(probs, vals[...], ((0,), (0,)))
        mine = jnp.concatenate([att[:lat, :HEAD], att[lat:, HEAD:]], axis=1).astype(BF16)
        wo = w_ref[:, 3].reshape(d, 128)
        o_ref[0] = dot(mine, wo, ((1,), (1,))).astype(BF16)


def attention(media_normed, state, gain, weights):
    s, t, d = media_normed.shape
    lat = state.shape[1]
    n = weights.shape[0]
    return pl.pallas_call(
        attention_kernel,
        grid=(s, t // CHUNK),
        in_specs=[
            pl.BlockSpec((1, CHUNK, d), lambda i, j: (i, j, 0)),
            pl.BlockSpec((1, lat, d), lambda i, j: (i, 0, 0)),
            pl.BlockSpec((1, d), lambda i, j: (0, 0)),
            pl.BlockSpec((n, 4, d // n, 128), lambda i, j: (0, 0, 0, 0)),
        ],
        out_specs=pl.BlockSpec((1, lat, d), lambda i, j: (i, 0, 0)),
        out_shape=jax.ShapeDtypeStruct((s, lat, d), BF16),
        scratch_shapes=[
            pltpu.VMEM((d, 256), BF16),
            pltpu.VMEM((128, 2 * lat), BF16),
            pltpu.VMEM((t + lat, 2 * lat), F32),
            pltpu.VMEM((t + lat, 128), BF16),
        ],
        compiler_params=params(),
        cost_estimate=pl.CostEstimate(flops=6 * 10**9, bytes_accessed=10 * 2**20, transcendentals=10**6),
        name="attention",
    )(media_normed, state, gain.reshape(1, d), weights)


def ffn_kernel(x_ref, s_ref, g_ref, a_ref, b_ref, c_ref, d_ref, e_ref, o_ref, f_ref):
    rows, d = s_ref.shape
    q = d // 4
    f_ref[...] = norm(s_ref[...], g_ref[...]).astype(BF16)
    x = x_ref[0]
    pieces = ((0, 0, a_ref), (3, 0, b_ref), (1, 0, c_ref), (2, 0, d_ref), (2, 1, e_ref))
    at = []
    for step, half, ref in pieces:
        n = ref.shape[1] * ref.shape[2]
        at.append((pl.multiple_of(lax.rem(x + step, 4) * q + half * (q // 2), q // 2), n))
    up = None
    for (lo, n), (_, _, ref) in zip(at, pieces):
        part = dot(f_ref[:, pl.ds(lo, n)], ref[0].reshape(n, ref.shape[3]))
        up = part if up is None else up + part
    hidden = (0.5 * up * (1.0 + lax.erf(up * (0.5**0.5)))).astype(BF16)
    for (lo, n), (_, _, ref) in zip(at, pieces):
        o_ref[:, pl.ds(lo, n)] = dot(hidden, ref[1].reshape(n, ref.shape[3]), ((1,), (1,))).astype(BF16)


def ffn(place, state, gain, pieces):
    rows, d = state.shape
    vmem = pl.BlockSpec(memory_space=pltpu.VMEM)
    return pl.pallas_call(
        ffn_kernel,
        in_specs=[pl.BlockSpec(memory_space=pltpu.SMEM)] + [vmem] * 7,
        out_specs=vmem,
        out_shape=jax.ShapeDtypeStruct((rows, d), BF16),
        scratch_shapes=[pltpu.VMEM((rows, d), BF16)],
        compiler_params=params(),
        cost_estimate=pl.CostEstimate(flops=2 * 10**9, bytes_accessed=5 * 2**20, transcendentals=10**5),
        name="ffn",
    )(place, state, gain.reshape(1, d), *pieces)


def ffn_weights(up, down_t):
    own = for_everyone(jnp.stack([up, down_t]), ("z", "yh"), 16)
    own = own.transpose(1, 0, 2, 3)
    right, left = ring_pairs(4, 1), ring_pairs(4, -1)
    a = lax.ppermute(own, "x", right)
    b = lax.ppermute(own, "x", left)
    c = lax.ppermute(a[:, :8], "x", right)
    e = lax.ppermute(b[:, 8:], "x", left)
    return own, a, b, c, e


def total(partial):
    core = lax.axis_index("c")
    swap = [(0, 1), (1, 0)]
    keep = lax.dynamic_index_in_dim(partial, core, 0, keepdims=False)
    give = lax.dynamic_index_in_dim(partial, 1 - core, 0, keepdims=False)
    got = lax.ppermute(give, "c", swap)
    half = (keep.astype(F32) + got.astype(F32)).astype(BF16)
    other = lax.ppermute(half, "yl", swap)
    full = (half.astype(F32) + other.astype(F32)).astype(BF16)
    theirs = lax.ppermute(full, "c", swap)
    first = jnp.where(core == 0, full, theirs)
    second = jnp.where(core == 0, theirs, full)
    return jnp.stack([first, second]).astype(F32)


def on_device(
    media, latents, time_embed, media_gain, latent_gain, ffn_gain, out_gain,
    w_query, w_key, w_value, w_out, w_up, w_down,
):
    samples, _, _, width = media.shape
    count = latents.shape[0]
    out_t = w_out.transpose(0, 2, 1)
    down_t = w_down.transpose(0, 2, 1)
    place = lax.axis_index("x").astype(jnp.int32).reshape(1)
    heads = [
        for_everyone(jnp.stack([w_query[n], w_key[n], w_value[n], out_t[n]]), DP, 64).reshape(64, 4, 16, 128)
        for n in range(LAYERS)
    ]
    pieces = [ffn_weights(w_up[n], down_t[n]) for n in range(LAYERS)]
    normed = norm_media(media, time_embed, media_gain)
    state = jnp.broadcast_to(latents.astype(F32)[None], (samples, count, width))
    for n in range(LAYERS):
        state = state + total(attention(normed[n], state, latent_gain[n], heads[n]))
        rows = state.reshape(samples * count, width)
        update = ffn(place, rows, ffn_gain[n], pieces[n])
        state = state + total(update.reshape(samples, count, width))
    return norm(state, out_gain).astype(BF16)


def solution(mesh):
    fine = Mesh(mesh.devices.reshape(4, 8, 2, 2, 2), ("x", "z", "yh", "yl", "c"))
    rows, cols = P(None, DP, MP), P(None, MP, DP)
    return jax.shard_map(
        on_device,
        mesh=fine,
        in_specs=(P(DP), P(), P(), P(), P(), P(), P(), rows, rows, rows, cols, rows, cols),
        out_specs=P(DP),
        check_vma=False,
    )
```

```python
import functools

import jax
import jax.numpy as jnp
from jax import lax
from jax.experimental import pallas as pl
from jax.experimental.pallas import tpu as pltpu
from jax.sharding import Mesh, PartitionSpec as P

HEAD = 64
LAYERS = 2
CHUNK = 512
F32, BF16 = jnp.float32, jnp.bfloat16
DP = ("x", "z", "yh")
MP = ("yl", "c")


def params(mib=58):
    return pltpu.CompilerParams(vmem_limit_bytes=mib * 1024 * 1024)


def norm(v, g):
    center = v - jnp.mean(v, axis=-1, keepdims=True)
    spread = jnp.mean(center * center, axis=-1, keepdims=True)
    return center * lax.rsqrt(spread + 1e-05) * g


def dot(a, b, dims=((1,), (0,))):
    return lax.dot_general(a, b, (dims, ((), ())), preferred_element_type=F32)


def ring_pairs(n, step):
    return [(i, (i + step) % n) for i in range(n)]


def pack_kernel(q_ref, k_ref, v_ref, o_ref, u_ref, d_ref, first_ref, second_ref, down_ref, first, second, down, in_sems, out_sems):
    def tiles(ref, n):
        return [ref.at[n, :, pl.ds(k, 128)] for k in range(0, ref.shape[2], 128)]

    parts = [ref.at[n] for n in range(LAYERS) for ref in (q_ref, k_ref, v_ref, o_ref)]
    loads = [(block, first.at[k]) for k, block in enumerate(parts + tiles(u_ref, 0))]
    loads += [(block, second.at[k]) for k, block in enumerate(tiles(u_ref, 1) + tiles(d_ref, 1))]
    loads += [(d_ref.at[0], down)]
    loads = [pltpu.make_async_copy(src, dst, in_sems.at[k]) for k, (src, dst) in enumerate(loads)]
    for copy in loads:
        copy.start()
    for copy in loads:
        copy.wait()
    stores = [(src, dst.at[k]) for src, dst in ((first, first_ref), (second, second_ref)) for k in range(16)]
    stores += [(down, down_ref)]
    stores = [pltpu.make_async_copy(src, dst, out_sems.at[k]) for k, (src, dst) in enumerate(stores)]
    for copy in stores:
        copy.start()
    for copy in stores:
        copy.wait()


def pack(wq, wk, wv, out_t, up, down_t):
    anywhere = pl.BlockSpec(memory_space=pl.ANY)
    copies = jax.ShapeDtypeStruct((16, 16, 16, 128), BF16)
    return pl.pallas_call(
        pack_kernel,
        in_specs=[anywhere] * 6,
        out_specs=[anywhere] * 3,
        out_shape=[copies, copies, jax.ShapeDtypeStruct(down_t.shape[1:], BF16)],
        scratch_shapes=[
            pltpu.VMEM((16, 16, 128), BF16),
            pltpu.VMEM((16, 16, 128), BF16),
            pltpu.VMEM(down_t.shape[1:], BF16),
            pltpu.SemaphoreType.DMA((33,)),
            pltpu.SemaphoreType.DMA((33,)),
        ],
        compiler_params=params(),
        name="pack",
    )(wq, wk, wv, out_t, up, down_t)


def x_order(x, pieces):
    out = []
    for step, half, ref in zip((0, 3, 1, 2, 2), (0, 0, 0, 0, 1), pieces):
        out.append((pl.ds(lax.rem(x + step, 4) * 16 + half * 8, ref.shape[0]), ref))
    return out


def media_kernel(m_ref, t_ref, o_ref, buf, embed, in_sems, out_sems):
    samples, frames, patches, d = buf.shape
    tiles = [slice(k, k + 128) for k in range(0, d, 128)]
    ones = jnp.ones((d, 128), BF16)
    rows = 128
    places = [(i, f) for i in range(samples) for f in range(frames)]
    for k, p in enumerate(places):
        pltpu.make_async_copy(m_ref.at[p], buf.at[p], in_sems.at[k]).start()

    embed[...] = t_ref[...].astype(F32)

    def load(k):
        i, f = k // frames, lax.rem(k, frames)
        return pltpu.make_async_copy(m_ref.at[i, f], buf.at[i, f], in_sems.at[k])

    def store(k):
        i, f = k // frames, lax.rem(k, frames)
        return pltpu.make_async_copy(buf.at[i, f], o_ref.at[i, f], out_sems.at[k])

    def frame_of(k, _):
        i, f = k // frames, lax.rem(k, frames)
        load(k).wait()
        frame = embed[pl.ds(f, 1), :]
        shift = jnp.sum(frame, axis=-1, keepdims=True)
        for lo in range(0, patches, rows):
            at = slice(lo, lo + rows)
            mean = (dot(buf[i, f, at, :], ones) + shift) * (1.0 / d)
            spread = None
            for t in tiles:
                c = buf[i, f, at, t].astype(F32) + frame[:, t] - mean
                spread = c * c if spread is None else spread + c * c
            scale = lax.rsqrt(jnp.sum(spread, axis=-1, keepdims=True) * (1.0 / d) + 1e-05)
            for t in tiles:
                unit = (buf[i, f, at, t].astype(F32) + frame[:, t] - mean) * scale
                buf[i, f, at, t] = unit.astype(BF16)
        store(k).start()
        return 0

    lax.fori_loop(0, len(places), frame_of, 0)

    def stored(k, _):
        store(k).wait()
        return 0

    lax.fori_loop(0, len(places), stored, 0)


def norm_media(media, time_embed):
    s, f, p, d = media.shape
    anywhere = pl.BlockSpec(memory_space=pl.ANY)
    return pl.pallas_call(
        media_kernel,
        in_specs=[anywhere, pl.BlockSpec(memory_space=pltpu.VMEM)],
        out_specs=anywhere,
        out_shape=jax.ShapeDtypeStruct(media.shape, BF16),
        scratch_shapes=[
            pltpu.VMEM(media.shape, BF16),
            pltpu.VMEM(time_embed.shape, F32),
            pltpu.SemaphoreType.DMA((s * f,)),
            pltpu.SemaphoreType.DMA((s * f,)),
        ],
        compiler_params=params(),
        cost_estimate=pl.CostEstimate(flops=3 * 10**9, bytes_accessed=16 * 2**20, transcendentals=0),
        name="norm_media",
    )(media, time_embed).reshape(s, f * p, d)


def attention_kernel(layer, at_ref, m_ref, s_ref, g_ref, mg_ref, *refs):
    pieces, refs = refs[:5], refs[5:]
    updated = layer > 0
    if updated:
        mine_ref, theirs_ref, *refs = refs
    keep_ref, give_ref, new_ref, wide, kv_w, score, vals = refs
    samples, tokens, d = m_ref.shape
    lat = new_ref.shape[1]
    for rows, ref in x_order(at_ref[0], pieces):
        for k in range(4):
            wide[k, rows] = ref[:, 4 * layer + k]
    gain = jnp.broadcast_to(mg_ref[layer : layer + 1, :], (128, d)).T

    def w(k):
        return wide[k].reshape(d, 128)

    for k in range(2):
        kv_w[:, k * 128 : (k + 1) * 128] = (w(1 + k).astype(F32) * gain).astype(BF16)
    core = at_ref[3]
    row = lax.broadcasted_iota(jnp.int32, (128, 2 * lat), 0) < HEAD
    col = lax.broadcasted_iota(jnp.int32, (128, 2 * lat), 1) < lat
    for i in range(samples):
        if updated:
            state = s_ref[i] + jnp.where(core == i, mine_ref[...].astype(F32), theirs_ref[...].astype(F32))
        else:
            state = s_ref[...].astype(F32)
        new_ref[i] = state
        ln = norm(state, g_ref[layer : layer + 1, :]).astype(BF16)
        q = (dot(ln, w(0)) * (HEAD**-0.5)).astype(BF16).astype(F32)
        qt = q.T
        q_bd = jnp.where(row == col, jnp.concatenate([qt, qt], axis=1), 0.0).astype(BF16)
        score[i, tokens:, :] = dot(dot(ln, w(1)).astype(BF16), q_bd)
        vals[i, tokens:, :] = dot(ln, w(2)).astype(BF16)

        for lo in range(0, tokens, CHUNK):
            at = slice(lo, lo + CHUNK)
            kv = dot(m_ref[i, at, :], kv_w[...]).astype(BF16)
            score[i, at, :] = dot(kv[:, :128], q_bd)
            vals[i, at, :] = kv[:, 128:]
    for i in range(samples):
        sc = score[i]
        e = jnp.exp(sc - jnp.max(sc, axis=0, keepdims=True))
        probs = (e * (1.0 / jnp.sum(e, axis=0, keepdims=True))).astype(BF16)
        att = dot(probs, vals[i], ((0,), (0,)))
        mine = jnp.concatenate([att[:lat, :HEAD], att[lat:, HEAD:]], axis=1).astype(BF16)
        out = dot(mine, w(3), ((1,), (1,))).astype(BF16)

        @pl.when(core == i)
        def _():
            keep_ref[...] = out

        @pl.when(core != i)
        def _():
            give_ref[...] = out


def attention(layer, places, media_normed, state, update, gain, media_gain, pieces):
    s, t, d = media_normed.shape
    lat = state.shape[-2]
    half = jax.ShapeDtypeStruct((lat, d), BF16)
    vmem = pl.BlockSpec(memory_space=pltpu.VMEM)
    return pl.pallas_call(
        functools.partial(attention_kernel, layer),
        in_specs=[pl.BlockSpec(memory_space=pltpu.SMEM)] + [vmem] * (9 + len(update)),
        out_specs=[vmem] * 3,
        out_shape=[half, half, jax.ShapeDtypeStruct((s, lat, d), F32)],
        scratch_shapes=[
            pltpu.VMEM((4, d // 16, 16, 128), BF16),
            pltpu.VMEM((d, 256), BF16),
            pltpu.VMEM((s, t + lat, 2 * lat), F32),
            pltpu.VMEM((s, t + lat, 128), BF16),
        ],
        compiler_params=params(24),
        cost_estimate=pl.CostEstimate(flops=6 * 10**9, bytes_accessed=10 * 2**20, transcendentals=10**6),
        name="attention",
    )(places, media_normed, state, gain, media_gain, *pieces, *update)


def ffn_kernel(layer, n_x, at_ref, s_ref, mine_ref, theirs_ref, g_ref, *refs):
    pieces, (keep_ref, give_ref, new_ref, u_ref, d_ref, o_ref) = refs[:-6], refs[-6:]
    rows, d = s_ref.shape
    hid = u_ref.shape[2]
    lat = rows // 2
    x, z, y, core = (at_ref[k] for k in range(4))
    tiles = [pl.ds(k, 128) for k in range(0, hid, 128)]
    order = x_order(x, pieces[:5])
    for at, ref in order:
        for k, tile in enumerate(tiles):
            u_ref[at, :, tile] = ref[:, k]
            if n_x == 16:
                d_ref[at, :, tile] = ref[:, 8 + k]
    for step, lo, ref in zip((0, 7, 1, 6, 2, 5, 3, 4, 4), (0,) * 8 + (2,), pieces[5:]):
        for i in range(ref.shape[0]):
            far = lax.rem(x + (0, 3, 1, 2)[lo + i], 4) * 8 + lax.rem(z + step, 8)
            for k in range(2):
                d_ref[far * 2 + (y if k == 0 else 1 - y)] = ref[i, k]
    here = pl.ds(pl.multiple_of(core * lat, lat), lat)
    there = pl.ds(pl.multiple_of((1 - core) * lat, lat), lat)
    new_ref[here, :] = s_ref[here, :] + mine_ref[...].astype(F32)
    new_ref[there, :] = s_ref[there, :] + theirs_ref[...].astype(F32)
    normed = norm(new_ref[...], g_ref[layer : layer + 1, :]).astype(BF16)
    up = dot(normed, u_ref[...].reshape(d, hid))
    hidden = (0.5 * up * (1.0 + lax.erf(up * (0.5**0.5)))).astype(BF16)
    o_ref[...] = dot(hidden, d_ref[...].reshape(d, hid), ((1,), (1,))).astype(BF16)
    keep_ref[...] = o_ref[here, :]
    give_ref[...] = o_ref[there, :]


def ffn(layer, places, state, update, gain, pieces):
    rows, d = state.shape
    vmem = pl.BlockSpec(memory_space=pltpu.VMEM)
    half = jax.ShapeDtypeStruct((rows // 2, d), BF16)
    return pl.pallas_call(
        functools.partial(ffn_kernel, layer, pieces[0].shape[1]),
        in_specs=[pl.BlockSpec(memory_space=pltpu.SMEM)] + [vmem] * (4 + len(pieces)),
        out_specs=[vmem] * 3,
        out_shape=[half, half, jax.ShapeDtypeStruct((rows, d), F32)],
        scratch_shapes=[
            pltpu.VMEM((d // 16, 16, 1024), BF16),
            pltpu.VMEM((d // 16, 16, 1024), BF16),
            pltpu.VMEM((rows, d), BF16),
        ],
        compiler_params=params(24),
        cost_estimate=pl.CostEstimate(flops=2 * 10**9, bytes_accessed=5 * 2**20, transcendentals=10**5),
        name="ffn",
    )(places, state, *update, gain, *pieces)


def x_ring(own):
    right, left = ring_pairs(4, 1), ring_pairs(4, -1)
    half = own.shape[0] // 2
    a, b = lax.ppermute(own, "x", right), lax.ppermute(own, "x", left)
    c, e = lax.ppermute(a[:half], "x", right), lax.ppermute(b[half:], "x", left)
    return own, a, b, c, e


def z_ring(own):
    right, left = ring_pairs(8, 1), ring_pairs(8, -1)
    half = own.shape[0] // 2
    pieces, r, l = [own], own, own
    for _ in range(3):
        r, l = lax.ppermute(r, "z", right), lax.ppermute(l, "z", left)
        pieces += [r, l]
    pieces += [lax.ppermute(r[:half], "z", right), lax.ppermute(l[half:], "z", left)]
    return pieces


def down_pieces(own):
    other = lax.ppermute(own, "yh", [(0, 1), (1, 0)])
    line = x_ring(jnp.stack([own, other]))
    return z_ring(jnp.concatenate([*line[:3], *line[3:]]).reshape(4, 2, *own.shape))


def total(keep, give):
    swap = [(0, 1), (1, 0)]
    got = lax.ppermute(give, "c", swap)
    half = (keep.astype(F32) + got.astype(F32)).astype(BF16)
    other = lax.ppermute(half, "yl", swap)
    full = (half.astype(F32) + other.astype(F32)).astype(BF16)
    return full, lax.ppermute(full, "c", swap)


def on_device(
    media, latents, time_embed, media_gain, latent_gain, ffn_gain, out_gain,
    w_query, w_key, w_value, w_out, w_up, w_down,
):
    samples, _, _, width = media.shape
    count = latents.shape[0]
    out_t = w_out.transpose(0, 2, 1)
    down_t = w_down.transpose(0, 2, 1)
    places = jnp.stack([lax.axis_index(k) for k in ("x", "z", "yh", "c")]).astype(jnp.int32)
    first, second, down = pack(w_query, w_key, w_value, out_t, w_up, down_t)
    first = lax.all_to_all(first, ("z", "yh"), 0, 0, tiled=True)
    down = down_pieces(down)
    heads = x_ring(first[:, :8])
    second = lax.all_to_all(second, ("z", "yh"), 0, 0, tiled=True)
    pieces = [(*x_ring(first[:, 8:]), *down), x_ring(second)]
    normed = norm_media(media, time_embed)
    state, update = latents, ()
    for n in range(LAYERS):
        keep, give, state = attention(n, places, normed, state, update, latent_gain, media_gain, heads)
        update = total(keep, give)
        rows = state.reshape(samples * count, width)
        keep, give, rows = ffn(n, places, rows, update, ffn_gain, pieces[n])
        state = rows.reshape(state.shape)
        update = total(keep, give)
    own = places[3] == 0
    added = jnp.stack([jnp.where(own, *update), jnp.where(own, *update[::-1])])
    return norm(state + added.astype(F32), out_gain).astype(BF16)


def solution(mesh):
    fine = Mesh(mesh.devices.reshape(4, 8, 2, 2, 2), ("x", "z", "yh", "yl", "c"))
    rows, cols = P(None, DP, MP), P(None, MP, DP)
    return jax.shard_map(
        on_device,
        mesh=fine,
        in_specs=(P(DP), P(), P(), P(), P(), P(), P(), rows, rows, rows, cols, rows, cols),
        out_specs=P(DP),
        check_vma=False,
    )
```

```python
import functools

import jax
import jax.numpy as jnp
from jax import lax
from jax.experimental import pallas as pl
from jax.experimental.pallas import tpu as pltpu
from jax.sharding import Mesh, PartitionSpec as P

HEAD = 64
LAYERS = 2
CHUNK = 512
F32, BF16 = jnp.float32, jnp.bfloat16
DP = ("x", "z", "yh")
MP = ("yl", "c")


def params(mib=58):
    return pltpu.CompilerParams(vmem_limit_bytes=mib * 1024 * 1024)


def norm(v, g):
    center = v - jnp.mean(v, axis=-1, keepdims=True)
    spread = jnp.mean(center * center, axis=-1, keepdims=True)
    return center * lax.rsqrt(spread + 1e-05) * g


def dot(a, b, dims=((1,), (0,))):
    return lax.dot_general(a, b, (dims, ((), ())), preferred_element_type=F32)


def ring_pairs(n, step):
    return [(i, (i + step) % n) for i in range(n)]


def pack_kernel(q_ref, k_ref, v_ref, o_ref, u_ref, d_ref, first_ref, second_ref, down_ref, first, second, down, in_sems, out_sems):
    def tiles(ref, n):
        return [ref.at[n, :, pl.ds(k, 128)] for k in range(0, ref.shape[2], 128)]

    parts = [ref.at[n] for n in range(LAYERS) for ref in (q_ref, k_ref, v_ref, o_ref)]
    loads = [(block, first.at[k]) for k, block in enumerate(parts + tiles(u_ref, 0))]
    loads += [(block, second.at[k]) for k, block in enumerate(tiles(u_ref, 1) + tiles(d_ref, 1))]
    loads += [(d_ref.at[0], down)]
    loads = [pltpu.make_async_copy(src, dst, in_sems.at[k]) for k, (src, dst) in enumerate(loads)]
    for copy in loads:
        copy.start()
    for copy in loads:
        copy.wait()
    stores = [(src, dst.at[k]) for src, dst in ((first, first_ref), (second, second_ref)) for k in range(16)]
    stores += [(down, down_ref)]
    stores = [pltpu.make_async_copy(src, dst, out_sems.at[k]) for k, (src, dst) in enumerate(stores)]
    for copy in stores:
        copy.start()
    for copy in stores:
        copy.wait()


def pack(wq, wk, wv, out_t, up, down_t):
    anywhere = pl.BlockSpec(memory_space=pl.ANY)
    copies = jax.ShapeDtypeStruct((16, 16, 16, 128), BF16)
    return pl.pallas_call(
        pack_kernel,
        in_specs=[anywhere] * 6,
        out_specs=[anywhere] * 3,
        out_shape=[copies, copies, jax.ShapeDtypeStruct(down_t.shape[1:], BF16)],
        scratch_shapes=[
            pltpu.VMEM((16, 16, 128), BF16),
            pltpu.VMEM((16, 16, 128), BF16),
            pltpu.VMEM(down_t.shape[1:], BF16),
            pltpu.SemaphoreType.DMA((33,)),
            pltpu.SemaphoreType.DMA((33,)),
        ],
        compiler_params=params(),
        name="pack",
    )(wq, wk, wv, out_t, up, down_t)


def x_order(x, pieces):
    out = []
    for k, ref in enumerate(pieces):
        far = lax.rem(x + (0, 3, 1, 2, 2)[k], 4) * 16
        out.append((pl.ds(far + 8 if k == 4 else far, ref.shape[0]), ref))
    return out


def media_kernel(m_ref, t_ref, o_ref, buf, embed, in_sems, out_sems):
    samples, frames, patches, d = buf.shape
    tiles = [slice(k, k + 128) for k in range(0, d, 128)]
    ones = jnp.ones((d, 128), BF16)
    rows = 128
    places = [(i, f) for i in range(samples) for f in range(frames)]
    for k, p in enumerate(places):
        pltpu.make_async_copy(m_ref.at[p], buf.at[p], in_sems.at[k]).start()

    embed[...] = t_ref[...].astype(F32)

    def load(k):
        i, f = k // frames, lax.rem(k, frames)
        return pltpu.make_async_copy(m_ref.at[i, f], buf.at[i, f], in_sems.at[k])

    def store(k):
        i, f = k // frames, lax.rem(k, frames)
        return pltpu.make_async_copy(buf.at[i, f], o_ref.at[i, f], out_sems.at[k])

    def frame_of(k, _):
        i, f = k // frames, lax.rem(k, frames)
        load(k).wait()
        frame = embed[pl.ds(f, 1), :]
        shift = jnp.sum(frame, axis=-1, keepdims=True)
        for lo in range(0, patches, rows):
            at = slice(lo, lo + rows)
            mean = (dot(buf[i, f, at, :], ones) + shift) * (1.0 / d)
            spread = None
            for t in tiles:
                c = buf[i, f, at, t].astype(F32) + frame[:, t] - mean
                spread = c * c if spread is None else spread + c * c
            scale = lax.rsqrt(jnp.sum(spread, axis=-1, keepdims=True) * (1.0 / d) + 1e-05)
            for t in tiles:
                unit = (buf[i, f, at, t].astype(F32) + frame[:, t] - mean) * scale
                buf[i, f, at, t] = unit.astype(BF16)
        store(k).start()
        return 0

    lax.fori_loop(0, len(places), frame_of, 0)

    def stored(k, _):
        store(k).wait()
        return 0

    lax.fori_loop(0, len(places), stored, 0)


def norm_media(media, time_embed):
    s, f, p, d = media.shape
    anywhere = pl.BlockSpec(memory_space=pl.ANY)
    return pl.pallas_call(
        media_kernel,
        in_specs=[anywhere, pl.BlockSpec(memory_space=pltpu.VMEM)],
        out_specs=anywhere,
        out_shape=jax.ShapeDtypeStruct(media.shape, BF16),
        scratch_shapes=[
            pltpu.VMEM(media.shape, BF16),
            pltpu.VMEM(time_embed.shape, F32),
            pltpu.SemaphoreType.DMA((s * f,)),
            pltpu.SemaphoreType.DMA((s * f,)),
        ],
        compiler_params=params(),
        cost_estimate=pl.CostEstimate(flops=3 * 10**9, bytes_accessed=16 * 2**20, transcendentals=0),
        name="norm_media",
    )(media, time_embed).reshape(s, f * p, d)


def attention_kernel(layer, at_ref, m_ref, s_ref, g_ref, mg_ref, *refs):
    pieces, refs = refs[:4], refs[4:]
    updated = layer > 0
    if updated:
        mine_ref, theirs_ref, *refs = refs
    keep_ref, give_ref, new_ref, wide, kv_w, score, vals = refs
    samples, tokens, d = m_ref.shape
    lat = new_ref.shape[1]
    for rows, ref in x_order(at_ref[0], pieces):
        for k in range(4):
            wide[k, rows] = ref[:, k]
    gain = jnp.broadcast_to(mg_ref[layer : layer + 1, :], (128, d)).T

    def w(k):
        return wide[k].reshape(d, 128)

    for k in range(2):
        kv_w[:, k * 128 : (k + 1) * 128] = (w(1 + k).astype(F32) * gain).astype(BF16)
    core = at_ref[3]
    row = lax.broadcasted_iota(jnp.int32, (128, 2 * lat), 0) < HEAD
    col = lax.broadcasted_iota(jnp.int32, (128, 2 * lat), 1) < lat

    def fill(i, _):
        if updated:
            state = s_ref[i] + jnp.where(core == i, mine_ref[...].astype(F32), theirs_ref[...].astype(F32))
        else:
            state = s_ref[...].astype(F32)
        new_ref[i] = state
        ln = norm(state, g_ref[layer : layer + 1, :]).astype(BF16)
        q = (dot(ln, w(0)) * (HEAD**-0.5)).astype(BF16).astype(F32)
        qt = q.T
        q_bd = jnp.where(row == col, jnp.concatenate([qt, qt], axis=1), 0.0).astype(BF16)
        score[i, tokens:, :] = dot(dot(ln, w(1)).astype(BF16), q_bd)
        vals[i, tokens:, :] = dot(ln, w(2)).astype(BF16)
        for lo in range(0, tokens, CHUNK):
            at = slice(lo, lo + CHUNK)
            kv = dot(m_ref[i, at, :], kv_w[...]).astype(BF16)
            score[i, at, :] = dot(kv[:, :128], q_bd)
            vals[i, at, :] = kv[:, 128:]
        return 0

    lax.fori_loop(0, samples, fill, 0)

    def attend(i, _):
        sc = score[i]
        e = jnp.exp(sc - jnp.max(sc, axis=0, keepdims=True))
        probs = (e * (1.0 / jnp.sum(e, axis=0, keepdims=True))).astype(BF16)
        att = dot(probs, vals[i], ((0,), (0,)))
        mine = jnp.concatenate([att[:lat, :HEAD], att[lat:, HEAD:]], axis=1).astype(BF16)
        out = dot(mine, w(3), ((1,), (1,))).astype(BF16)

        @pl.when(core == i)
        def _():
            keep_ref[...] = out

        @pl.when(core != i)
        def _():
            give_ref[...] = out

        return 0

    lax.fori_loop(0, samples, attend, 0)


def attention(layer, places, media_normed, state, update, gain, media_gain, pieces):
    s, t, d = media_normed.shape
    lat = state.shape[-2]
    half = jax.ShapeDtypeStruct((lat, d), BF16)
    vmem = pl.BlockSpec(memory_space=pltpu.VMEM)
    return pl.pallas_call(
        functools.partial(attention_kernel, layer),
        in_specs=[pl.BlockSpec(memory_space=pltpu.SMEM)] + [vmem] * (8 + len(update)),
        out_specs=[vmem] * 3,
        out_shape=[half, half, jax.ShapeDtypeStruct((s, lat, d), F32)],
        scratch_shapes=[
            pltpu.VMEM((4, d // 16, 16, 128), BF16),
            pltpu.VMEM((d, 256), BF16),
            pltpu.VMEM((s, t + lat, 2 * lat), F32),
            pltpu.VMEM((s, t + lat, 128), BF16),
        ],
        compiler_params=params(24),
        cost_estimate=pl.CostEstimate(flops=6 * 10**9, bytes_accessed=10 * 2**20, transcendentals=10**6),
        name="attention",
    )(places, media_normed, state, gain, media_gain, *pieces, *update)


def ffn_kernel(layer, n_x, at_ref, s_ref, mine_ref, theirs_ref, g_ref, *refs):
    n_up = 5 if n_x == 16 else 4
    ups, downs, refs = refs[:n_up], refs[n_up:-6], refs[-6:]
    (keep_ref, give_ref, new_ref, u_ref, d_ref, o_ref) = refs
    rows, d = s_ref.shape
    hid = u_ref.shape[2]
    lat = rows // 2
    x, z, y, core = (at_ref[k] for k in range(4))
    tiles = [pl.ds(k, 128) for k in range(0, hid, 128)]
    order = x_order(x, ups)
    for at, ref in order:
        for k, tile in enumerate(tiles):
            u_ref[at, :, tile] = ref[:, k]
            if n_x == 16:
                d_ref[at, :, tile] = ref[:, 8 + k]
    for step, ref in zip((0, 7, 1, 6, 2, 5, 3, 4), downs):
        for i in range(4):
            far = lax.rem(x + (0, 3, 1, 2)[i], 4) * 8 + lax.rem(z + step, 8)
            for k in range(2):
                d_ref[far * 2 + (y if k == 0 else 1 - y)] = ref[i, k]
    here = pl.ds(pl.multiple_of(core * lat, lat), lat)
    there = pl.ds(pl.multiple_of((1 - core) * lat, lat), lat)
    new_ref[here, :] = s_ref[here, :] + mine_ref[...].astype(F32)
    new_ref[there, :] = s_ref[there, :] + theirs_ref[...].astype(F32)
    normed = norm(new_ref[...], g_ref[layer : layer + 1, :]).astype(BF16)
    up = dot(normed, u_ref[...].reshape(d, hid))
    hidden = (0.5 * up * (1.0 + lax.erf(up * (0.5**0.5)))).astype(BF16)
    o_ref[...] = dot(hidden, d_ref[...].reshape(d, hid), ((1,), (1,))).astype(BF16)
    keep_ref[...] = o_ref[here, :]
    give_ref[...] = o_ref[there, :]


def ffn(layer, places, state, update, gain, pieces):
    rows, d = state.shape
    vmem = pl.BlockSpec(memory_space=pltpu.VMEM)
    half = jax.ShapeDtypeStruct((rows // 2, d), BF16)
    return pl.pallas_call(
        functools.partial(ffn_kernel, layer, pieces[0].shape[1]),
        in_specs=[pl.BlockSpec(memory_space=pltpu.SMEM)] + [vmem] * (4 + len(pieces)),
        out_specs=[vmem] * 3,
        out_shape=[half, half, jax.ShapeDtypeStruct((rows, d), F32)],
        scratch_shapes=[
            pltpu.VMEM((d // 16, 16, 1024), BF16),
            pltpu.VMEM((d // 16, 16, 1024), BF16),
            pltpu.VMEM((rows, d), BF16),
        ],
        compiler_params=params(24),
        cost_estimate=pl.CostEstimate(flops=2 * 10**9, bytes_accessed=5 * 2**20, transcendentals=10**5),
        name="ffn",
    )(places, state, *update, gain, *pieces)


def x_ring(own):
    right, left = ring_pairs(4, 1), ring_pairs(4, -1)
    half = own.shape[0] // 2
    a, b = lax.ppermute(own, "x", right), lax.ppermute(own, "x", left)
    c, e = lax.ppermute(a[:half], "x", right), lax.ppermute(b[half:], "x", left)
    return own, a, b, c, e


def x_direct(own):
    return [own] + [lax.ppermute(own, "x", ring_pairs(4, step)) for step in (1, -1, 2)]


def z_ring(own):
    right, left = ring_pairs(8, 1), ring_pairs(8, -1)
    pieces, r, l = [own], own, own
    for k in range(4):
        r = lax.ppermute(r, "z", right)
        pieces.append(r)
        if k < 3:
            l = lax.ppermute(l, "z", left)
            pieces.append(l)
    return pieces


def down_pieces(own):
    other = lax.ppermute(own, "yh", [(0, 1), (1, 0)])
    line = x_direct(jnp.stack([own, other]))
    return z_ring(jnp.stack(line))


def total(keep, give):
    swap = [(0, 1), (1, 0)]
    got = lax.ppermute(give, "c", swap)
    half = (keep.astype(F32) + got.astype(F32)).astype(BF16)
    other = lax.ppermute(half, "yl", swap)
    full = (half.astype(F32) + other.astype(F32)).astype(BF16)
    return full, lax.ppermute(full, "c", swap)


def on_device(
    media, latents, time_embed, media_gain, latent_gain, ffn_gain, out_gain,
    w_query, w_key, w_value, w_out, w_up, w_down,
):
    samples, _, _, width = media.shape
    count = latents.shape[0]
    out_t = w_out.transpose(0, 2, 1)
    down_t = w_down.transpose(0, 2, 1)
    places = jnp.stack([lax.axis_index(k) for k in ("x", "z", "yh", "c")]).astype(jnp.int32)
    first, second, down = pack(w_query, w_key, w_value, out_t, w_up, down_t)
    first = lax.all_to_all(first, ("z", "yh"), 0, 0, tiled=True)
    down = down_pieces(down)
    heads = [x_direct(first[:, 4 * n : 4 * n + 4]) for n in range(LAYERS)]
    second = lax.all_to_all(second, ("z", "yh"), 0, 0, tiled=True)
    pieces = [(*x_direct(first[:, 8:]), *down), x_ring(second)]
    normed = norm_media(media, time_embed)
    state, update = latents, ()
    for n in range(LAYERS):
        keep, give, state = attention(n, places, normed, state, update, latent_gain, media_gain, heads[n])
        update = total(keep, give)
        rows = state.reshape(samples * count, width)
        keep, give, rows = ffn(n, places, rows, update, ffn_gain, pieces[n])
        state = rows.reshape(state.shape)
        update = total(keep, give)
    own = places[3] == 0
    added = jnp.stack([jnp.where(own, *update), jnp.where(own, *update[::-1])])
    return norm(state + added.astype(F32), out_gain).astype(BF16)


def solution(mesh):
    fine = Mesh(mesh.devices.reshape(4, 8, 2, 2, 2), ("x", "z", "yh", "yl", "c"))
    rows, cols = P(None, DP, MP), P(None, MP, DP)
    return jax.shard_map(
        on_device,
        mesh=fine,
        in_specs=(P(DP), P(), P(), P(), P(), P(), P(), rows, rows, rows, cols, rows, cols),
        out_specs=P(DP),
        check_vma=False,
    )
```

```python
import functools

import jax
import jax.numpy as jnp
from jax import lax
from jax.experimental import pallas as pl
from jax.experimental.pallas import tpu as pltpu
from jax.sharding import Mesh, PartitionSpec as P

HEAD = 64
LAYERS = 2
CHUNK = 2048
F32, BF16 = jnp.float32, jnp.bfloat16
DP = ("x", "z", "yh")
MP = ("yl", "c")


def params(mib=58):
    return pltpu.CompilerParams(vmem_limit_bytes=mib * 1024 * 1024)


def norm(v, g):
    center = v - jnp.mean(v, axis=-1, keepdims=True)
    spread = jnp.mean(center * center, axis=-1, keepdims=True)
    return center * lax.rsqrt(spread + 1e-05) * g


def dot(a, b, dims=((1,), (0,))):
    return lax.dot_general(a, b, (dims, ((), ())), preferred_element_type=F32)


def ring_pairs(n, step):
    return [(i, (i + step) % n) for i in range(n)]


def pack_kernel(q_ref, k_ref, v_ref, o_ref, u_ref, d_ref, first_ref, second_ref, down_ref, first, second, down, in_sems, out_sems):
    def tiles(ref, n):
        return [ref.at[n, :, pl.ds(k, 128)] for k in range(0, ref.shape[2], 128)]

    parts = [ref.at[n] for n in range(LAYERS) for ref in (q_ref, k_ref, v_ref, o_ref)]
    loads = [(block, first.at[k]) for k, block in enumerate(parts + tiles(u_ref, 0))]
    loads += [(block, second.at[k]) for k, block in enumerate(tiles(u_ref, 1) + tiles(d_ref, 1))]
    loads += [(d_ref.at[0], down)]
    loads = [pltpu.make_async_copy(src, dst, in_sems.at[k]) for k, (src, dst) in enumerate(loads)]
    for copy in loads:
        copy.start()
    for copy in loads:
        copy.wait()
    stores = [(src, dst.at[k]) for src, dst in ((first, first_ref), (second, second_ref)) for k in range(16)]
    stores += [(down, down_ref)]
    stores = [pltpu.make_async_copy(src, dst, out_sems.at[k]) for k, (src, dst) in enumerate(stores)]
    for copy in stores:
        copy.start()
    for copy in stores:
        copy.wait()


def pack(wq, wk, wv, out_t, up, down_t):
    anywhere = pl.BlockSpec(memory_space=pl.ANY)
    copies = jax.ShapeDtypeStruct((16, 16, 16, 128), BF16)
    return pl.pallas_call(
        pack_kernel,
        in_specs=[anywhere] * 6,
        out_specs=[anywhere] * 3,
        out_shape=[copies, copies, jax.ShapeDtypeStruct(down_t.shape[1:], BF16)],
        scratch_shapes=[
            pltpu.VMEM((16, 16, 128), BF16),
            pltpu.VMEM((16, 16, 128), BF16),
            pltpu.VMEM(down_t.shape[1:], BF16),
            pltpu.SemaphoreType.DMA((33,)),
            pltpu.SemaphoreType.DMA((33,)),
        ],
        compiler_params=params(),
        name="pack",
    )(wq, wk, wv, out_t, up, down_t)


def x_order(x, pieces):
    out = []
    for k, ref in enumerate(pieces):
        far = lax.rem(x + (0, 3, 1, 2, 2)[k], 4) * 16
        out.append((pl.ds(far + 8 if k == 4 else far, ref.shape[0]), ref))
    return out


def media_kernel(m_ref, t_ref, o_ref, buf, embed, in_sems, out_sems):
    samples, frames, patches, d = buf.shape
    tiles = [slice(k, k + 128) for k in range(0, d, 128)]
    ones = jnp.ones((d, 128), BF16)
    rows = 128
    places = [(i, f) for i in range(samples) for f in range(frames)]
    for k, p in enumerate(places):
        pltpu.make_async_copy(m_ref.at[p], buf.at[p], in_sems.at[k]).start()

    embed[...] = t_ref[...].astype(F32)

    def load(k):
        i, f = k // frames, lax.rem(k, frames)
        return pltpu.make_async_copy(m_ref.at[i, f], buf.at[i, f], in_sems.at[k])

    def store(k):
        i, f = k // frames, lax.rem(k, frames)
        return pltpu.make_async_copy(buf.at[i, f], o_ref.at[i, f], out_sems.at[k])

    def frame_of(k, _):
        i, f = k // frames, lax.rem(k, frames)
        load(k).wait()
        frame = embed[pl.ds(f, 1), :]
        shift = jnp.sum(frame, axis=-1, keepdims=True)
        for lo in range(0, patches, rows):
            at = slice(lo, lo + rows)
            mean = (dot(buf[i, f, at, :], ones) + shift) * (1.0 / d)
            spread = None
            for t in tiles:
                c = buf[i, f, at, t].astype(F32) + frame[:, t] - mean
                spread = c * c if spread is None else spread + c * c
            scale = lax.rsqrt(jnp.sum(spread, axis=-1, keepdims=True) * (1.0 / d) + 1e-05)
            for t in tiles:
                unit = (buf[i, f, at, t].astype(F32) + frame[:, t] - mean) * scale
                buf[i, f, at, t] = unit.astype(BF16)
        store(k).start()
        return 0

    lax.fori_loop(0, len(places), frame_of, 0)

    def stored(k, _):
        store(k).wait()
        return 0

    lax.fori_loop(0, len(places), stored, 0)


def norm_media(media, time_embed):
    s, f, p, d = media.shape
    anywhere = pl.BlockSpec(memory_space=pl.ANY)
    return pl.pallas_call(
        media_kernel,
        in_specs=[anywhere, pl.BlockSpec(memory_space=pltpu.VMEM)],
        out_specs=anywhere,
        out_shape=jax.ShapeDtypeStruct(media.shape, BF16),
        scratch_shapes=[
            pltpu.VMEM(media.shape, BF16),
            pltpu.VMEM(time_embed.shape, F32),
            pltpu.SemaphoreType.DMA((s * f,)),
            pltpu.SemaphoreType.DMA((s * f,)),
        ],
        compiler_params=params(),
        cost_estimate=pl.CostEstimate(flops=3 * 10**9, bytes_accessed=16 * 2**20, transcendentals=0),
        name="norm_media",
    )(media, time_embed).reshape(s, f * p, d)


def attention_kernel(layer, at_ref, m_ref, s_ref, g_ref, mg_ref, *refs):
    pieces, refs = refs[:4], refs[4:]
    updated = layer > 0
    if updated:
        mine_ref, theirs_ref, *refs = refs
    keep_ref, give_ref, new_ref, wide, kv_w, score, vals = refs
    samples, tokens, d = m_ref.shape
    lat = new_ref.shape[1]
    for rows, ref in x_order(at_ref[0], pieces):
        for k in range(4):
            wide[k, rows] = ref[:, k]
    gain = jnp.broadcast_to(mg_ref[layer : layer + 1, :], (128, d)).T

    def w(k):
        return wide[k].reshape(d, 128)

    for k in range(2):
        kv_w[:, k * 128 : (k + 1) * 128] = (w(1 + k).astype(F32) * gain).astype(BF16)
    core = at_ref[3]
    row = lax.broadcasted_iota(jnp.int32, (128, 2 * lat), 0) < HEAD
    col = lax.broadcasted_iota(jnp.int32, (128, 2 * lat), 1) < lat

    def fill(i, _):
        if updated:
            state = s_ref[i] + jnp.where(core == i, mine_ref[...].astype(F32), theirs_ref[...].astype(F32))
        else:
            state = s_ref[...].astype(F32)
        new_ref[i] = state
        ln = norm(state, g_ref[layer : layer + 1, :]).astype(BF16)
        q = (dot(ln, w(0)) * (HEAD**-0.5)).astype(BF16).astype(F32)
        qt = q.T
        q_bd = jnp.where(row == col, jnp.concatenate([qt, qt], axis=1), 0.0).astype(BF16)
        score[i, tokens:, :] = dot(dot(ln, w(1)).astype(BF16), q_bd)
        vals[i, tokens:, :] = dot(ln, w(2)).astype(BF16)
        for lo in range(0, tokens, CHUNK):
            at = slice(lo, lo + CHUNK)
            kv = dot(m_ref[i, at, :], kv_w[...]).astype(BF16)
            score[i, at, :] = dot(kv[:, :128], q_bd)
            vals[i, at, :] = kv[:, 128:]
        return 0

    lax.fori_loop(0, samples, fill, 0)

    def attend(i, _):
        sc = score[i]
        e = jnp.exp(sc - jnp.max(sc, axis=0, keepdims=True))
        probs = (e * (1.0 / jnp.sum(e, axis=0, keepdims=True))).astype(BF16)
        att = dot(probs, vals[i], ((0,), (0,)))
        mine = jnp.concatenate([att[:lat, :HEAD], att[lat:, HEAD:]], axis=1).astype(BF16)
        out = dot(mine, w(3), ((1,), (1,))).astype(BF16)

        @pl.when(core == i)
        def _():
            keep_ref[...] = out

        @pl.when(core != i)
        def _():
            give_ref[...] = out

        return 0

    lax.fori_loop(0, samples, attend, 0)


def attention(layer, places, media_normed, state, update, gain, media_gain, pieces):
    s, t, d = media_normed.shape
    lat = state.shape[-2]
    half = jax.ShapeDtypeStruct((lat, d), BF16)
    vmem = pl.BlockSpec(memory_space=pltpu.VMEM)
    return pl.pallas_call(
        functools.partial(attention_kernel, layer),
        in_specs=[pl.BlockSpec(memory_space=pltpu.SMEM)] + [vmem] * (8 + len(update)),
        out_specs=[vmem] * 3,
        out_shape=[half, half, jax.ShapeDtypeStruct((s, lat, d), F32)],
        scratch_shapes=[
            pltpu.VMEM((4, d // 16, 16, 128), BF16),
            pltpu.VMEM((d, 256), BF16),
            pltpu.VMEM((s, t + lat, 2 * lat), F32),
            pltpu.VMEM((s, t + lat, 128), BF16),
        ],
        compiler_params=params(16),
        cost_estimate=pl.CostEstimate(flops=6 * 10**9, bytes_accessed=10 * 2**20, transcendentals=10**6),
        name="attention",
    )(places, media_normed, state, gain, media_gain, *pieces, *update)


def ffn_kernel(layer, n_x, at_ref, s_ref, mine_ref, theirs_ref, g_ref, *refs):
    n_up = 5 if n_x == 16 else 4
    ups, downs, refs = refs[:n_up], refs[n_up:-6], refs[-6:]
    (keep_ref, give_ref, new_ref, u_ref, d_ref, o_ref) = refs
    rows, d = s_ref.shape
    hid = u_ref.shape[2]
    lat = rows // 2
    x, z, y, core = (at_ref[k] for k in range(4))
    tiles = [pl.ds(k, 128) for k in range(0, hid, 128)]
    order = x_order(x, ups)
    for at, ref in order:
        for k, tile in enumerate(tiles):
            u_ref[at, :, tile] = ref[:, k]
            if n_x == 16:
                d_ref[at, :, tile] = ref[:, 8 + k]
    for step, ref in zip((0, 7, 1, 6, 2, 5, 3, 4), downs):
        for i in range(4):
            far = lax.rem(x + (0, 3, 1, 2)[i], 4) * 8 + lax.rem(z + step, 8)
            for k in range(2):
                d_ref[far * 2 + (y if k == 0 else 1 - y)] = ref[i, k]
    here = pl.ds(pl.multiple_of(core * lat, lat), lat)
    there = pl.ds(pl.multiple_of((1 - core) * lat, lat), lat)
    new_ref[here, :] = s_ref[here, :] + mine_ref[...].astype(F32)
    new_ref[there, :] = s_ref[there, :] + theirs_ref[...].astype(F32)
    normed = norm(new_ref[...], g_ref[layer : layer + 1, :]).astype(BF16)
    up = dot(normed, u_ref[...].reshape(d, hid))
    hidden = (0.5 * up * (1.0 + lax.erf(up * (0.5**0.5)))).astype(BF16)
    o_ref[...] = dot(hidden, d_ref[...].reshape(d, hid), ((1,), (1,))).astype(BF16)
    keep_ref[...] = o_ref[here, :]
    give_ref[...] = o_ref[there, :]


def ffn(layer, places, state, update, gain, pieces):
    rows, d = state.shape
    vmem = pl.BlockSpec(memory_space=pltpu.VMEM)
    half = jax.ShapeDtypeStruct((rows // 2, d), BF16)
    return pl.pallas_call(
        functools.partial(ffn_kernel, layer, pieces[0].shape[1]),
        in_specs=[pl.BlockSpec(memory_space=pltpu.SMEM)] + [vmem] * (4 + len(pieces)),
        out_specs=[vmem] * 3,
        out_shape=[half, half, jax.ShapeDtypeStruct((rows, d), F32)],
        scratch_shapes=[
            pltpu.VMEM((d // 16, 16, 1024), BF16),
            pltpu.VMEM((d // 16, 16, 1024), BF16),
            pltpu.VMEM((rows, d), BF16),
        ],
        compiler_params=params(14),
        cost_estimate=pl.CostEstimate(flops=2 * 10**9, bytes_accessed=5 * 2**20, transcendentals=10**5),
        name="ffn",
    )(places, state, *update, gain, *pieces)


def x_ring(own):
    right, left = ring_pairs(4, 1), ring_pairs(4, -1)
    half = own.shape[0] // 2
    a, b = lax.ppermute(own, "x", right), lax.ppermute(own, "x", left)
    c, e = lax.ppermute(a[:half], "x", right), lax.ppermute(b[half:], "x", left)
    return own, a, b, c, e


def x_direct(own):
    return [own] + [lax.ppermute(own, "x", ring_pairs(4, step)) for step in (1, -1, 2)]


def z_ring(own):
    right, left = ring_pairs(8, 1), ring_pairs(8, -1)
    pieces, r, l = [own], own, own
    for k in range(4):
        r = lax.ppermute(r, "z", right)
        pieces.append(r)
        if k < 3:
            l = lax.ppermute(l, "z", left)
            pieces.append(l)
    return pieces


def down_pieces(own):
    other = lax.ppermute(own, "yh", [(0, 1), (1, 0)])
    line = x_direct(jnp.stack([own, other]))
    return z_ring(jnp.stack(line))


def total(keep, give):
    swap = [(0, 1), (1, 0)]
    got = lax.ppermute(give, "c", swap)
    half = (keep.astype(F32) + got.astype(F32)).astype(BF16)
    other = lax.ppermute(half, "yl", swap)
    full = (half.astype(F32) + other.astype(F32)).astype(BF16)
    return full, lax.ppermute(full, "c", swap)


def on_device(
    media, latents, time_embed, media_gain, latent_gain, ffn_gain, out_gain,
    w_query, w_key, w_value, w_out, w_up, w_down,
):
    samples, _, _, width = media.shape
    count = latents.shape[0]
    out_t = w_out.transpose(0, 2, 1)
    down_t = w_down.transpose(0, 2, 1)
    places = jnp.stack([lax.axis_index(k) for k in ("x", "z", "yh", "c")]).astype(jnp.int32)
    first, second, down = pack(w_query, w_key, w_value, out_t, w_up, down_t)
    first = lax.all_to_all(first, ("z", "yh"), 0, 0, tiled=True)
    down = down_pieces(down)
    heads = [x_direct(first[:, 4 * n : 4 * n + 4]) for n in range(LAYERS)]
    second = lax.all_to_all(second, ("z", "yh"), 0, 0, tiled=True)
    pieces = [(*x_direct(first[:, 8:]), *down), x_ring(second)]
    normed = norm_media(media, time_embed)
    state, update = latents, ()
    for n in range(LAYERS):
        keep, give, state = attention(n, places, normed, state, update, latent_gain, media_gain, heads[n])
        update = total(keep, give)
        rows = state.reshape(samples * count, width)
        keep, give, rows = ffn(n, places, rows, update, ffn_gain, pieces[n])
        state = rows.reshape(state.shape)
        update = total(keep, give)
    own = places[3] == 0
    added = jnp.stack([jnp.where(own, *update), jnp.where(own, *update[::-1])])
    return norm(state + added.astype(F32), out_gain).astype(BF16)


def solution(mesh):
    fine = Mesh(mesh.devices.reshape(4, 8, 2, 2, 2), ("x", "z", "yh", "yl", "c"))
    rows, cols = P(None, DP, MP), P(None, MP, DP)
    return jax.shard_map(
        on_device,
        mesh=fine,
        in_specs=(P(DP), P(), P(), P(), P(), P(), P(), rows, rows, rows, cols, rows, cols),
        out_specs=P(DP),
        check_vma=False,
    )
```
